256 devices in a mesh: front: 32 (over z, x), panel: 8 (over y, core).
Axes of the slice: x: 4, y: 4, z: 8, core: 2. Of those that a mesh axis runs over, the one named last changes fastest.
Arguments:
- coupling: bfloat16 [32, 2048, 2048], P('front', 'panel'), may hold values from -1 to 1
- pivot_inverse: bfloat16 [32, 2048, 2048], P('front', 'panel'), may hold values from -0.125 to 0.125
- pivots: float32 [32, 2048], P('front'), as said below
- trailing: float32 [32, 2048, 2048], P('front', 'panel'), may hold values from -12 to 12
- sketch: float32 [32, 8, 8, 32, 256], P('front', 'panel'), may hold values from -6 to 6
- extend_map: int32 [32, 2048], replicated, may hold values from 0 to 511, as said below
- parent_of: int32 [32], replicated, may hold values from 0 to 31, as said below
- parent_base: bfloat16 [32, 4096, 4096], P('front', 'panel'), may hold values from -6 to 6
Outputs:
- assembled: bfloat16 [32, 4096, 4096], P('front', 'panel')
The draws below stay inside these ranges and needn't reach their ends.
Inputs may be any that keep to these rules, and one draw needn't show every extreme that they name: `extend_map`: within each front and each aligned block of 2048 / 8 entries the values are distinct and rising. `pivots`: every entry's magnitude lies between 0.5 and 2 times 2048 ** -0.5; signs are mixed. `parent_of`: no parent has more than 4 children; some parent has exactly 4.
All inputs are finite; a program needn't handle non-finite values.
Results may differ from the reference program's by a relative error of at most 0.0043.
Values may be sent and summed in bfloat16 or wider, within the bound.
A program may use at most 128 MiB of HBM per device.

```python
import jax
import jax.numpy as jnp
from jax import lax

NP = 2048
NC = 2048
PORDER = 4096
TILE = 256
RANK = 32
MAXKIDS = 4
FRONTS = 32
N_PANEL = 8


def draw_pivots(key, part):
    sign_key, size_key = jax.random.split(jax.random.fold_in(key, 11))
    signs = jnp.where(jax.random.bernoulli(sign_key, 0.5, (FRONTS, NP)), 1.0, -1.0).astype(jnp.float32)
    magnitude = jnp.exp(jax.random.uniform(size_key, (FRONTS, NP), jnp.float32, jnp.log(0.5), jnp.log(2.0)))
    return (signs * magnitude / jnp.sqrt(jnp.float32(NP))).astype(jnp.float32)


def draw_extend_map(key, part):
    row_dev = NC // N_PANEL
    parent_dev = PORDER // N_PANEL
    keys = jax.random.split(jax.random.fold_in(key, 23), FRONTS * N_PANEL)

    def one_block(block_key):
        chosen = jax.random.permutation(block_key, parent_dev)[:row_dev]
        return jnp.sort(chosen).astype(jnp.int32)
    blocks = jax.vmap(one_block)(keys)
    return blocks.reshape(FRONTS, NC).astype(jnp.int32)


def draw_parent_of(key, part):
    base = jax.random.fold_in(key, 41)
    order_key, full_key, rest_key = jax.random.split(base, 3)
    full_parent = jax.random.randint(full_key, (), 0, FRONTS).astype(jnp.int32)
    other_slots = jnp.arange((FRONTS - 1) * MAXKIDS, dtype=jnp.int32) // MAXKIDS
    other_slots = other_slots + (other_slots >= full_parent).astype(jnp.int32)
    shuffled = jax.random.permutation(rest_key, other_slots)
    listing = jnp.concatenate([jnp.full((MAXKIDS,), 1, jnp.int32) * full_parent, shuffled[:FRONTS - MAXKIDS]])
    placing = jax.random.permutation(order_key, FRONTS).astype(jnp.int32)
    return listing[placing].astype(jnp.int32)


def draw_coupling(key, part):
    base = jax.random.fold_in(key, 31)
    tile_rows = NC // TILE
    decay = 1.5 * RANK
    spectrum = jnp.exp(-jnp.arange(TILE, dtype=jnp.float32) / decay)
    scale = jnp.sqrt(jnp.sum(spectrum * spectrum) * NP)

    def one_tile(index):
        left_key, right_key = jax.random.split(jax.random.fold_in(base, index))
        left = jax.random.normal(left_key, (TILE, TILE), jnp.float32)
        right = jax.random.normal(right_key, (TILE, NP), jnp.float32)
        return jnp.dot(left * spectrum[None, :], right, precision=lax.Precision.HIGHEST) / scale
    blocks = lax.map(one_tile, jnp.arange(FRONTS * tile_rows, dtype=jnp.int32))
    return blocks.reshape(FRONTS, NC, NP).astype(jnp.bfloat16)


def draw_trailing(key, part):
    base = jax.random.fold_in(key, 37)
    tile_rows = NC // TILE
    decay = 0.75 * RANK
    spectrum = jnp.exp(-jnp.arange(TILE, dtype=jnp.float32) / decay)
    scale = jnp.sqrt(jnp.sum(spectrum * spectrum))

    def one_tile(index):
        left_key, right_key = jax.random.split(jax.random.fold_in(base, index))
        left = jax.random.normal(left_key, (TILE, TILE), jnp.float32)
        right = jax.random.normal(right_key, (TILE, TILE), jnp.float32)
        return jnp.dot(left * spectrum[None, :], right, precision=lax.Precision.HIGHEST) / scale
    blocks = lax.map(one_tile, jnp.arange(FRONTS * tile_rows * tile_rows, dtype=jnp.int32))
    blocks = blocks.reshape(FRONTS, tile_rows, tile_rows, TILE, TILE)
    return jnp.transpose(blocks, (0, 1, 3, 2, 4)).reshape(FRONTS, NC, NC).astype(jnp.float32)


def level_of(own_key, shape, cuts, smallest, largest):
    def one(axis_at, shards_of):
        steps = jax.random.uniform(jax.random.fold_in(jax.random.fold_in(own_key, 6), axis_at), (shards_of,), jnp.float32, smallest / len(cuts), largest / len(cuts))
        return jnp.repeat(jnp.exp(steps), shape[axis_at] // shards_of).reshape((-1,) + (1,) * (len(shape) - axis_at - 1))

    level = one(*cuts[0])
    for cut in cuts[1:]:
        level = level * one(*cut)
    return level


def bell_draw(stream_key, shape, scale, reach, cuts=(), kind=jnp.bfloat16):
    array = scale * jax.random.normal(stream_key, shape, jnp.float32)
    if cuts:
        array = array * level_of(stream_key, shape, cuts, -0.22, 0.18)
    return jnp.clip(array, -reach, reach).astype(kind)


def setup_inputs(seed: int = 0) -> dict:
    seeds = jax.random.split(jax.random.key(seed), 9)
    return {
        "coupling": draw_coupling(jax.random.fold_in(seeds[8], 71), 0),
        "pivot_inverse": bell_draw(seeds[1], (FRONTS, NP, NP), NP ** -0.5, 0.125, ((0, 32), (1, 8))),
        "pivots": draw_pivots(jax.random.fold_in(seeds[8], 71), 0),
        "trailing": draw_trailing(jax.random.fold_in(seeds[8], 71), 0),
        "sketch": bell_draw(seeds[4], (FRONTS, NC // TILE, NC // TILE, RANK, TILE), 1.0, 6.0, ((0, 32), (1, 8)), jnp.float32),
        "extend_map": draw_extend_map(jax.random.fold_in(seeds[8], 71), 0),
        "parent_of": draw_parent_of(jax.random.fold_in(seeds[8], 71), 0),
        "parent_base": bell_draw(seeds[7], (FRONTS, PORDER, PORDER), 1.0, 6.0, ((0, 32), (1, 8))),
    }


def compress(schur, omega):
    tiles = schur.reshape(NC // TILE, TILE, NC // TILE, TILE)
    range_t = jnp.einsum('ijkb,iajb->ijka', omega, tiles, precision=lax.Precision.HIGHEST)
    gram = jnp.einsum('ijka,ijla->ijkl', range_t, range_t, precision=lax.Precision.HIGHEST)
    lower = jnp.linalg.cholesky(gram)
    basis = jax.scipy.linalg.solve_triangular(lower, range_t, lower=True)
    coeff = jnp.einsum('ijka,iajb->ijkb', basis, tiles, precision=lax.Precision.HIGHEST)
    return (basis.astype(jnp.bfloat16), coeff.astype(jnp.bfloat16))

def expand(basis, coeff):
    dense = jnp.einsum('ijka,ijkb->iajb', basis.astype(jnp.float32), coeff.astype(jnp.float32))
    return dense.reshape(NC, NC)

def reference(coupling, pivot_inverse, pivots, trailing, sketch, extend_map, parent_of, parent_base):
    row_dev = NC // N_PANEL
    parent_dev = PORDER // N_PANEL

    def child(carry, inputs):
        coupling_f, inverse_f, pivots_f, trailing_f, sketch_f = inputs
        factor = jnp.dot(coupling_f.astype(jnp.float32), inverse_f.astype(jnp.float32), preferred_element_type=jnp.float32).astype(jnp.bfloat16)
        scaled = (factor.astype(jnp.float32) / pivots_f[None, :]).astype(jnp.bfloat16)
        update = lax.dot_general(scaled.astype(jnp.float32), factor.astype(jnp.float32), (((1,), (1,)), ((), ())), preferred_element_type=jnp.float32)
        basis, coeff = compress(trailing_f - update, sketch_f)
        return (carry, (basis, coeff))
    _, (basis_all, coeff_all) = lax.scan(child, jnp.int32(0), (coupling, pivot_inverse, pivots, trailing, sketch))
    positions = jnp.arange(NC, dtype=jnp.int32)
    global_map = (positions // row_dev * parent_dev)[None, :] + extend_map.astype(jnp.int32)

    def parent(carry, target):

        def add_child(front_idx, total):

            def place(acc):
                where = global_map[front_idx]
                return acc.at[where[:, None], where[None, :]].add(expand(basis_all[front_idx], coeff_all[front_idx]))
            return lax.cond(parent_of[front_idx] == target, place, lambda acc: acc, total)
        start = parent_base[target].astype(jnp.float32)
        total = lax.fori_loop(0, FRONTS, add_child, start)
        return (carry, total.astype(jnp.bfloat16))
    _, assembled = lax.scan(parent, jnp.int32(0), jnp.arange(FRONTS, dtype=jnp.int32))
    return assembled
```

```python
import functools

import jax
import jax.numpy as jnp
from jax import lax
from jax.experimental import pallas as pl
from jax.experimental.pallas import tpu as pltpu
from jax.sharding import PartitionSpec as P

MAXKIDS = 4
HI = lax.Precision.HIGHEST


def dot(a, b, dims, precision=None):
    return lax.dot_general(
        a, b, (dims, ((), ())), precision=precision, preferred_element_type=jnp.float32
    )


def compress_kernel(schur_ref, omega_ref, basis_ref, coeff_ref):
    tiles, rank, tile = omega_ref.shape
    ys = []
    state = []
    row_id = lax.broadcasted_iota(jnp.int32, (rank, rank), 0)
    col_id = lax.broadcasted_iota(jnp.int32, (rank, rank), 1)
    eye = jnp.where(row_id == col_id, 1.0, 0.0).astype(jnp.float32)
    for j in range(tiles):
        block = schur_ref[:, j * tile:(j + 1) * tile]
        y = dot(omega_ref[j], block, ((1,), (1,)), HI)
        ys.append(y)
        state.append(jnp.concatenate([dot(y, y, ((1,), (1,)), HI), eye], axis=1))
    a = jnp.stack(state)
    rows = lax.broadcasted_iota(jnp.int32, (tiles, rank, 1), 1)
    for k in range(rank):
        pivot = a[:, k:k + 1, :]
        inverse = 1.0 / a[:, k:k + 1, k:k + 1]
        step = jnp.where(rows > k, a[:, :, k:k + 1] * inverse, 0.0)
        a = a - step * pivot
    for j in range(tiles):
        diag = jnp.sum(jnp.where(row_id == col_id, a[j, :, :rank], 0.0), axis=1, keepdims=True)
        inverse = a[j, :, rank:] * (1.0 / jnp.sqrt(diag))
        basis = dot(inverse, ys[j], ((1,), (0,)), HI)
        block = schur_ref[:, j * tile:(j + 1) * tile]
        basis_ref[j] = basis.astype(jnp.bfloat16)
        coeff_ref[j] = dot(basis, block, ((1,), (0,)), HI).astype(jnp.bfloat16)


def compress(schur, omega):
    tiles, rank, tile = omega.shape
    out = jax.ShapeDtypeStruct((tiles, rank, tile), jnp.bfloat16)
    return pl.pallas_call(
        compress_kernel,
        out_shape=(out, out),
        name="compress",
        compiler_params=pltpu.CompilerParams(vmem_limit_bytes=48 * 1024 * 1024),
    )(schur, omega)


def place_kernel(rowmap_ref, colmap_ref, basis_ref, coeff_ref, base_ref, out_ref, rt_ref):
    kids, _, tiles, rank, tile = basis_ref.shape
    height = out_ref.shape[1]
    width = out_ref.shape[2]
    j = pl.program_id(0)
    lanes = lax.broadcasted_iota(jnp.int32, (tile, width), 1)

    @pl.when(j == 0)
    def _():
        high = lax.broadcasted_iota(jnp.int32, (tile, height), 1)
        for s in range(kids):
            hot = jnp.where(rowmap_ref[:, s:s + 1] == high, 1.0, 0.0).astype(jnp.bfloat16)
            rt_ref[s] = dot(
                basis_ref[s, 0].reshape(tiles * rank, tile), hot, ((1,), (0,))
            ).astype(jnp.bfloat16)

    left = []
    right = []
    for s in range(kids):
        hot = jnp.where(colmap_ref[0, :, s:s + 1] == lanes, 1.0, 0.0).astype(jnp.bfloat16)
        right.append(dot(coeff_ref[s, 0, 0], hot, ((1,), (0,))).astype(jnp.bfloat16))
        left.append(rt_ref[s, pl.ds(j * rank, rank), :])
    left = jnp.concatenate(left, axis=0)
    right = jnp.concatenate(right, axis=0)
    total = dot(left, right, ((0,), (0,)))
    out_ref[0] = (base_ref[0].astype(jnp.float32) + total).astype(jnp.bfloat16)


def place(rowmap, colmap, data, base):
    kids, _, tiles, rank, tile = data.shape
    _, height, total = base.shape
    width = total // tiles
    return pl.pallas_call(
        place_kernel,
        grid=(tiles,),
        in_specs=[
            pl.BlockSpec((tile, kids), lambda j: (0, 0)),
            pl.BlockSpec((1, tile, kids), lambda j: (j, 0, 0)),
            pl.BlockSpec((kids, 1, tiles, rank, tile), lambda j: (0, 0, 0, 0, 0)),
            pl.BlockSpec((kids, 1, 1, rank, tile), lambda j: (0, 1, j, 0, 0)),
            pl.BlockSpec((1, height, width), lambda j: (0, 0, j)),
        ],
        out_specs=pl.BlockSpec((1, height, width), lambda j: (0, 0, j)),
        out_shape=jax.ShapeDtypeStruct(base.shape, base.dtype),
        scratch_shapes=[pltpu.VMEM((kids, tiles * rank, height), jnp.bfloat16)],
        name="place",
        compiler_params=pltpu.CompilerParams(vmem_limit_bytes=48 * 1024 * 1024),
    )(rowmap, colmap, data, data, base)


def family(parent_of):
    fronts = parent_of.shape[0]
    front_ids = jnp.arange(fronts, dtype=jnp.int32)
    same_parent = parent_of[:, None] == parent_of[None, :]
    position = jnp.sum(
        jnp.where(same_parent & (front_ids[None, :] < front_ids[:, None]), 1, 0), axis=1
    ).astype(jnp.int32)
    slot_ids = jnp.arange(MAXKIDS, dtype=jnp.int32)
    matches = (parent_of[None, :, None] == front_ids[:, None, None]) & (
        position[None, :, None] == slot_ids[None, None, :]
    )
    children = jnp.sum(jnp.where(matches, front_ids[None, :, None], 0), axis=1)
    present = jnp.any(matches, axis=1)
    return children, present


def body(coupling, pivot_inverse, pivots, trailing, sketch, extend_map, parent_of, parent_base):
    rows_here = coupling[0]
    row_dev = rows_here.shape[0]
    factor_sum = jnp.dot(
        rows_here,
        lax.all_gather(pivot_inverse, "panel", axis=1, tiled=True)[0],
        preferred_element_type=jnp.float32,
    )
    factor = factor_sum.astype(jnp.bfloat16)
    scaled = (factor.astype(jnp.float32) / pivots[0][None, :]).astype(jnp.bfloat16)
    gathered = lax.all_gather(factor, "panel", axis=0, tiled=True)
    update = dot(scaled, gathered, ((1,), (1,)))
    schur = trailing[0] - update
    basis, coeff = compress(schur, sketch[0, 0])

    panels = lax.axis_size("panel")
    owner = lax.axis_index("front")
    panel_here = lax.axis_index("panel")
    fronts = parent_of.shape[0]
    children, present = family(parent_of)
    packed = jnp.stack((basis, coeff)).reshape(fronts, -1)
    spread = lax.all_to_all(packed, "front", split_axis=0, concat_axis=0, tiled=True)
    chosen = jnp.take(spread, children.reshape(-1), axis=0)
    outgoing = jnp.where(present.reshape(-1)[:, None], chosen, jnp.zeros((), jnp.bfloat16)).reshape(
        fronts, MAXKIDS, -1
    )
    received = lax.all_to_all(outgoing, "front", split_axis=0, concat_axis=2, tiled=True)
    data = received[0].reshape((MAXKIDS, 2) + basis.shape)
    maps = jnp.where(present[owner][:, None], extend_map[children[owner]], -1)
    colmap = jnp.transpose(maps).reshape(panels, row_dev, MAXKIDS)
    rowmap = lax.dynamic_index_in_dim(colmap, panel_here, 0, keepdims=False)
    return place(rowmap, colmap, data, parent_base)


def solution(mesh):
    placed = (
        P("front", "panel", None),
        P("front", "panel", None),
        P("front", None),
        P("front", "panel", None),
        P("front", "panel", None, None, None),
        P(),
        P(),
        P("front", "panel", None),
    )
    return jax.shard_map(
        body, mesh=mesh, in_specs=placed, out_specs=P("front", "panel", None), check_vma=False
    )
```

```python
import functools

import jax
import jax.numpy as jnp
from jax import lax
from jax.experimental import pallas as pl
from jax.experimental.pallas import tpu as pltpu
from jax.sharding import PartitionSpec as P

MAXKIDS = 4
HI = lax.Precision.HIGHEST
MESH = pl.DeviceIdType.MESH


def dot(a, b, dims, precision=None):
    return lax.dot_general(
        a, b, (dims, ((), ())), precision=precision, preferred_element_type=jnp.float32
    )


def factor_kernel(steps, coupling_hbm, inverse_ref, pivots_ref, trailing_hbm, schur_ref,
                  coupling_ref, inverses, factors, scaled_ref, send_sem, recv_sem, local_sem):
    panel = lax.axis_index("panel")
    chip = panel // 2
    core = panel % 2
    other = 1 - core
    up = (chip + 1) % 4
    down = (chip + 3) % 4
    far = (chip + 2) % 4
    rows, cols = inverse_ref.shape
    half = rows // 2
    chunk = cols // steps
    partner = chip * 2 + other
    above = up * 2 + core
    below = down * 2 + core

    fetch_c = pltpu.make_async_copy(coupling_hbm, coupling_ref, local_sem.at[0])
    fetch_t = pltpu.make_async_copy(trailing_hbm, schur_ref, local_sem.at[1])
    fetch_w = pltpu.make_async_copy(inverse_ref, inverses.at[panel], local_sem.at[2])
    fetch_w.start()
    fetch_c.start()
    fetch_t.start()

    barrier = pltpu.get_barrier_semaphore()
    for target in (partner, above, below):
        pl.semaphore_signal(barrier, inc=1, device_id={"panel": target}, device_id_type=MESH)
    pl.semaphore_wait(barrier, 3)

    def view(phase, slot, part, c):
        buffer = factors if phase else inverses
        lanes = pl.ds(pl.multiple_of(c * chunk, chunk), chunk)
        if part == 0:
            return buffer.at[slot, :, lanes]
        return buffer.at[slot, pl.ds((part - 1) * half, half), lanes]

    mine = panel
    low = down * 2 + core
    high = up * 2 + core
    table = (
        (mine, 0, partner, partner),
        (mine, 0, above, low),
        (mine, 0, below, high),
        (low, 0, partner, down * 2 + other),
        (high, 0, partner, up * 2 + other),
        (low, 1, above, far * 2 + core),
        (high, 2, below, far * 2 + core),
        (far * 2 + core, 1, partner, far * 2 + other),
        (far * 2 + core, 2, partner, far * 2 + other),
    )

    def copy(phase, kind, c, source=None):
        slot, part, target, _ = table[kind]
        ref = view(phase, slot, part, c)
        return pltpu.make_async_remote_copy(
            src_ref=ref if source is None else source,
            dst_ref=ref,
            send_sem=send_sem.at[phase, c, kind],
            recv_sem=recv_sem.at[phase, c, kind],
            device_id={"panel": target},
            device_id_type=MESH,
        )

    def arrived(phase, kind, c):
        _, part, target, slot = table[kind]
        ref = view(phase, slot, part, c)
        pltpu.make_async_remote_copy(
            src_ref=ref,
            dst_ref=ref,
            send_sem=send_sem.at[phase, c, kind],
            recv_sem=recv_sem.at[phase, c, kind],
            device_id={"panel": target},
            device_id_type=MESH,
        ).wait_recv()

    def lanes_of(c):
        return pl.ds(pl.multiple_of(c * chunk, chunk), chunk)

    def send_inverse(c, carry):
        for kind in (1, 2, 0):
            copy(0, kind, c, inverse_ref.at[:, lanes_of(c)]).start()
        return carry

    def relay(phase, c):
        arrived(phase, 1, c)
        copy(phase, 5, c).start()
        copy(phase, 3, c).start()
        arrived(phase, 2, c)
        copy(phase, 6, c).start()
        copy(phase, 4, c).start()

    def relay_far(phase, c):
        arrived(phase, 5, c)
        copy(phase, 7, c).start()
        arrived(phase, 6, c)
        copy(phase, 8, c).start()

    def near_inverse(c, carry):
        relay(0, c)
        return carry

    def make_factor(c, carry):
        relay_far(0, c)
        for kind in (0, 3, 4, 7, 8):
            arrived(0, kind, c)
        lanes = lanes_of(c)
        total = dot(coupling_ref[:, :rows], inverses[0, :, lanes], ((1,), (0,)))
        for q in range(1, cols // rows):
            total = total + dot(
                coupling_ref[:, q * rows:(q + 1) * rows], inverses[q, :, lanes], ((1,), (0,))
            )
        factor = total.astype(jnp.bfloat16)
        factors[mine, :, lanes] = factor
        scaled_ref[:, lanes] = (factor.astype(jnp.float32) / pivots_ref[:, lanes]).astype(jnp.bfloat16)
        for kind in (1, 2, 0):
            copy(1, kind, c).start()
        return carry

    def apply(slot, c):
        lanes = lanes_of(c)
        out = pl.ds(pl.multiple_of(slot * rows, rows), rows)
        schur_ref[:, out] -= dot(scaled_ref[:, lanes], factors[slot, :, lanes], ((1,), (1,)))

    def near_factor(c, carry):
        apply(mine, c)
        arrived(1, 0, c)
        apply(partner, c)
        relay(1, c)
        apply(low, c)
        apply(high, c)
        arrived(1, 3, c)
        apply(down * 2 + other, c)
        arrived(1, 4, c)
        apply(up * 2 + other, c)
        return carry

    def far_factor(c, carry):
        relay_far(1, c)
        apply(far * 2 + core, c)
        arrived(1, 7, c)
        arrived(1, 8, c)
        apply(far * 2 + other, c)
        return carry

    lax.fori_loop(0, steps, send_inverse, 0)
    fetch_w.wait()
    fetch_c.wait()
    lax.fori_loop(0, steps, near_inverse, 0)
    lax.fori_loop(0, steps, make_factor, 0)
    fetch_t.wait()
    lax.fori_loop(0, steps, near_factor, 0)
    lax.fori_loop(0, steps, far_factor, 0)

    def drain(c, carry):
        for phase in range(2):
            for kind in range(9):
                copy(phase, kind, c).wait_send()
        return carry

    lax.fori_loop(0, steps, drain, 0)


def update(coupling, pivot_inverse, pivots, trailing):
    rows, cols = coupling.shape
    pieces = cols // rows
    steps = 4
    return pl.pallas_call(
        functools.partial(factor_kernel, steps),
        in_specs=[
            pl.BlockSpec(memory_space=pltpu.HBM),
            pl.BlockSpec(memory_space=pltpu.VMEM),
            pl.BlockSpec(memory_space=pltpu.VMEM),
            pl.BlockSpec(memory_space=pltpu.HBM),
        ],
        out_specs=pl.BlockSpec(memory_space=pltpu.VMEM),
        out_shape=jax.ShapeDtypeStruct(trailing.shape, trailing.dtype),
        scratch_shapes=[
            pltpu.VMEM((rows, cols), jnp.bfloat16),
            pltpu.VMEM((pieces, rows, cols), jnp.bfloat16),
            pltpu.VMEM((pieces, rows, cols), jnp.bfloat16),
            pltpu.VMEM((rows, cols), jnp.bfloat16),
            pltpu.SemaphoreType.DMA((2, steps, 9)),
            pltpu.SemaphoreType.DMA((2, steps, 9)),
            pltpu.SemaphoreType.DMA((3,)),
        ],
        name="update",
        compiler_params=pltpu.CompilerParams(
            collective_id=0, has_side_effects=True, vmem_limit_bytes=60 * 1024 * 1024
        ),
    )(coupling, pivot_inverse, pivots, trailing)


def compress_kernel(schur_ref, omega_ref, packed_ref):
    tiles, rank, tile = omega_ref.shape
    ys = []
    state = []
    row_id = lax.broadcasted_iota(jnp.int32, (rank, rank), 0)
    col_id = lax.broadcasted_iota(jnp.int32, (rank, rank), 1)
    eye = jnp.where(row_id == col_id, 1.0, 0.0).astype(jnp.float32)
    for j in range(tiles):
        block = schur_ref[:, j * tile:(j + 1) * tile]
        y = dot(omega_ref[j], block, ((1,), (1,)), HI)
        ys.append(y)
        state.append(jnp.concatenate([dot(y, y, ((1,), (1,)), HI), eye], axis=1))
    a = jnp.stack(state)
    rows = lax.broadcasted_iota(jnp.int32, (tiles, rank, 1), 1)
    for k in range(rank):
        pivot = a[:, k:k + 1, :]
        inverse = 1.0 / a[:, k:k + 1, k:k + 1]
        step = jnp.where(rows > k, a[:, :, k:k + 1] * inverse, 0.0)
        a = a - step * pivot
    for j in range(tiles):
        diag = jnp.sum(jnp.where(row_id == col_id, a[j, :, :rank], 0.0), axis=1, keepdims=True)
        inverse = a[j, :, rank:] * (1.0 / jnp.sqrt(diag))
        basis = dot(inverse, ys[j], ((1,), (0,)), HI)
        block = schur_ref[:, j * tile:(j + 1) * tile]
        packed_ref[j, :rank, :] = basis.astype(jnp.bfloat16)
        packed_ref[j, rank:, :] = dot(basis, block, ((1,), (0,)), HI).astype(jnp.bfloat16)


def compress(schur, omega):
    tiles, rank, tile = omega.shape
    out = jax.ShapeDtypeStruct((tiles, 2 * rank, tile), jnp.bfloat16)
    return pl.pallas_call(
        compress_kernel,
        out_shape=out,
        name="compress",
        compiler_params=pltpu.CompilerParams(vmem_limit_bytes=48 * 1024 * 1024),
    )(schur, omega)


class Exchange:
    def __init__(self, picks, packed, ring, staged, kids, sems):
        self.picks, self.packed, self.ring, self.staged, self.kids = picks, packed, ring, staged, kids
        self.split_send, self.split_recv, self.ring_send, self.ring_recv, self.pick_send, self.pick_recv, self.own = sems
        front = lax.axis_index("front")
        self.z = front // 4
        self.x = front % 4
        chip = lax.axis_index("panel") // 2
        self.tiles = [pl.ds(pl.multiple_of(2 * ((chip + d) % 4), 2), 2) for d in (0, 3, 1, 2)]

    def across(self, step):
        return self.z * 4 + (self.x + step) % 4

    def greeted(self):
        z = self.z
        return [self.across(s) for s in (1, 2, 3)] + [
            ((z + 1) % 8) * 4 + self.x, ((z + 7) % 8) * 4 + self.x]

    def part(self, x):
        return pl.ds(pl.multiple_of(16 * x, 16), 16)

    def split(self, g, step):
        return pltpu.make_async_remote_copy(
            src_ref=self.packed.at[self.tiles[g], self.part((self.x + step) % 4), :],
            dst_ref=self.ring[g].at[self.z, self.x],
            send_sem=self.split_send.at[g, step - 1],
            recv_sem=self.split_recv.at[g, step - 1],
            device_id={"front": self.across(step)},
            device_id_type=MESH,
        )

    def split_own(self, g):
        return pltpu.make_async_copy(
            self.packed.at[self.tiles[g], self.part(self.x), :],
            self.ring[g].at[self.z, self.x],
            self.own.at[g],
        )

    def split_start(self, g):
        for step in (2, 1, 3):
            self.split(g, step).start()
        self.split_own(g).start()

    def split_wait(self, g):
        self.split_own(g).wait()
        for step in (1, 3, 2):
            ref = self.ring[g].at[self.z, (self.x + 4 - step) % 4]
            pltpu.make_async_remote_copy(
                src_ref=ref,
                dst_ref=ref,
                send_sem=self.split_send.at[g, step - 1],
                recv_sem=self.split_recv.at[g, step - 1],
                device_id={"front": self.across(step)},
                device_id_type=MESH,
            ).wait_recv()

    def hop(self, g, way, k, incoming):
        sign = -1 if way == 0 else 1
        at = (self.z + 8 + sign * (k + incoming)) % 8
        ref = self.ring[g].at[at]
        if k == 3:
            ref = self.ring[g].at[at, pl.ds(2 * way, 2)]
        target = ((self.z + (1 if way == 0 else 7)) % 8) * 4 + self.x
        return pltpu.make_async_remote_copy(
            src_ref=ref,
            dst_ref=ref,
            send_sem=self.ring_send.at[g, way, k],
            recv_sem=self.ring_recv.at[g, way, k],
            device_id={"front": target},
            device_id_type=MESH,
        )

    def ring_start(self, g):
        self.split_wait(g)
        for way in (0, 1):
            self.hop(g, way, 0, 0).start()

    def ring_step(self, g, k):
        for way in (0, 1):
            self.hop(g, way, k - 1, 1).wait_recv()
            self.hop(g, way, k, 0).start()

    def ring_end(self, g):
        for way in (0, 1):
            self.hop(g, way, 3, 1).wait_recv()

    def pick(self, g, step):
        return pltpu.make_async_remote_copy(
            src_ref=self.staged.at[g, step - 1],
            dst_ref=self.kids.at[:, self.tiles[g], self.part(self.x), :],
            send_sem=self.pick_send.at[g, step - 1],
            recv_sem=self.pick_recv.at[g, step - 1],
            device_id={"front": self.across(step)},
            device_id_type=MESH,
        )

    def pick_start(self, g):
        for step in (2, 1, 3, 0):
            parent = self.across(step)
            for s in range(MAXKIDS):
                child = self.picks[parent, s]
                block = self.ring[g][child // 4, child % 4]
                if step:
                    self.staged[g, step - 1, s] = block
                else:
                    self.kids[s, self.tiles[g], self.part(self.x), :] = block
            if step:
                self.pick(g, step).start()

    def pick_wait(self, g):
        for step in (1, 3, 2):
            ref = self.kids.at[:, self.tiles[g], self.part((self.x + 4 - step) % 4), :]
            pltpu.make_async_remote_copy(
                src_ref=ref,
                dst_ref=ref,
                send_sem=self.pick_send.at[g, step - 1],
                recv_sem=self.pick_recv.at[g, step - 1],
                device_id={"front": self.across(step)},
                device_id_type=MESH,
            ).wait_recv()

    def drain(self, g):
        for step in (1, 2, 3):
            self.split(g, step).wait_send()
            self.pick(g, step).wait_send()
        for way in (0, 1):
            for k in range(4):
                self.hop(g, way, k, 0).wait_send()


def exchange_scratch():
    block = (2, 16, 256)
    return [
        pltpu.VMEM((4, 3, MAXKIDS) + block, jnp.bfloat16),
    ] + [pltpu.VMEM((8, 4) + block, jnp.bfloat16)] * 4 + [pltpu.SemaphoreType.DMA(shape) for shape in (
        (4, 3), (4, 3), (4, 2, 4), (4, 2, 4), (4, 3), (4, 3), (4,))]


def exchange_kernel(picks, packed, kids, staged, *rest):
    ex = Exchange(picks, packed, rest[:4], staged, kids, rest[4:])
    barrier = pltpu.get_barrier_semaphore()
    for target in ex.greeted():
        pl.semaphore_signal(barrier, inc=1, device_id={"front": target}, device_id_type=MESH)
    pl.semaphore_wait(barrier, 5)
    for g in range(4):
        ex.split_start(g)
    for g in (0, 1):
        ex.ring_start(g)
    for k in (1, 2, 3):
        for g in (0, 1):
            ex.ring_step(g, k)
    for g in (2, 3):
        ex.ring_start(g)
    for g in (0, 1):
        ex.ring_end(g)
        ex.pick_start(g)
    for k in (1, 2, 3):
        for g in (2, 3):
            ex.ring_step(g, k)
    for g in (2, 3):
        ex.ring_end(g)
        ex.pick_start(g)
    for g in range(4):
        ex.pick_wait(g)
    for g in range(4):
        ex.drain(g)


def exchange(picks, packed):
    tiles, depth, tile = packed.shape
    return pl.pallas_call(
        exchange_kernel,
        in_specs=[
            pl.BlockSpec(memory_space=pltpu.SMEM),
            pl.BlockSpec(memory_space=pltpu.VMEM),
        ],
        out_specs=pl.BlockSpec(memory_space=pltpu.VMEM),
        out_shape=jax.ShapeDtypeStruct((MAXKIDS, tiles, depth, tile), packed.dtype),
        scratch_shapes=exchange_scratch(),
        name="exchange",
        compiler_params=pltpu.CompilerParams(
            collective_id=1, has_side_effects=True, vmem_limit_bytes=48 * 1024 * 1024
        ),
    )(picks, packed)


def place_kernel(rowmap_ref, colmap_ref, basis_ref, coeff_ref, base_ref, out_ref, rt_ref):
    kids, tiles, rank, tile = basis_ref.shape
    height = out_ref.shape[1]
    width = out_ref.shape[2]
    j = pl.program_id(0)
    lanes = lax.broadcasted_iota(jnp.int32, (tile, width), 1)

    @pl.when(j == 0)
    def _():
        high = lax.broadcasted_iota(jnp.int32, (tile, height), 1)
        for s in range(kids):
            hot = jnp.where(rowmap_ref[:, s:s + 1] == high, 1.0, 0.0).astype(jnp.bfloat16)
            rt_ref[s] = dot(
                basis_ref[s].reshape(tiles * rank, tile), hot, ((1,), (0,))
            ).astype(jnp.bfloat16)

    left = []
    right = []
    for s in range(kids):
        hot = jnp.where(colmap_ref[0, :, s:s + 1] == lanes, 1.0, 0.0).astype(jnp.bfloat16)
        right.append(dot(coeff_ref[s, 0], hot, ((1,), (0,))).astype(jnp.bfloat16))
        left.append(rt_ref[s, pl.ds(j * rank, rank), :])
    left = jnp.concatenate(left, axis=0)
    right = jnp.concatenate(right, axis=0)
    total = dot(left, right, ((0,), (0,)))
    out_ref[0] = (base_ref[0].astype(jnp.float32) + total).astype(jnp.bfloat16)


def place(rowmap, colmap, data, base):
    kids, tiles, depth, tile = data.shape
    rank = depth // 2
    _, height, total = base.shape
    width = total // tiles
    return pl.pallas_call(
        place_kernel,
        grid=(tiles,),
        in_specs=[
            pl.BlockSpec((tile, kids), lambda j: (0, 0)),
            pl.BlockSpec((1, tile, kids), lambda j: (j, 0, 0)),
            pl.BlockSpec((kids, tiles, rank, tile), lambda j: (0, 0, 0, 0)),
            pl.BlockSpec((kids, 1, rank, tile), lambda j: (0, j, 1, 0)),
            pl.BlockSpec((1, height, width), lambda j: (0, 0, j)),
        ],
        out_specs=pl.BlockSpec((1, height, width), lambda j: (0, 0, j)),
        out_shape=jax.ShapeDtypeStruct(base.shape, base.dtype),
        scratch_shapes=[pltpu.VMEM((kids, tiles * rank, height), jnp.bfloat16)],
        name="place",
        compiler_params=pltpu.CompilerParams(vmem_limit_bytes=48 * 1024 * 1024),
    )(rowmap, colmap, data, data, base)


def family(parent_of):
    fronts = parent_of.shape[0]
    front_ids = jnp.arange(fronts, dtype=jnp.int32)
    same_parent = parent_of[:, None] == parent_of[None, :]
    position = jnp.sum(
        jnp.where(same_parent & (front_ids[None, :] < front_ids[:, None]), 1, 0), axis=1
    ).astype(jnp.int32)
    slot_ids = jnp.arange(MAXKIDS, dtype=jnp.int32)
    matches = (parent_of[None, :, None] == front_ids[:, None, None]) & (
        position[None, :, None] == slot_ids[None, None, :]
    )
    children = jnp.sum(jnp.where(matches, front_ids[None, :, None], 0), axis=1)
    present = jnp.any(matches, axis=1)
    return children, present


def body(coupling, pivot_inverse, pivots, trailing, sketch, extend_map, parent_of, parent_base):
    row_dev = coupling.shape[1]
    schur = update(coupling[0], pivot_inverse[0], pivots, trailing[0])
    packed = compress(schur, sketch[0, 0])

    panels = lax.axis_size("panel")
    owner = lax.axis_index("front")
    panel_here = lax.axis_index("panel")
    children, present = family(parent_of)
    data = exchange(children, packed)
    maps = jnp.where(present[owner][:, None], extend_map[children[owner]], -1)
    colmap = jnp.transpose(maps).reshape(panels, row_dev, MAXKIDS)
    rowmap = lax.dynamic_index_in_dim(colmap, panel_here, 0, keepdims=False)
    return place(rowmap, colmap, data, parent_base)


def solution(mesh):
    placed = (
        P("front", "panel", None),
        P("front", "panel", None),
        P("front", None),
        P("front", "panel", None),
        P("front", "panel", None, None, None),
        P(),
        P(),
        P("front", "panel", None),
    )
    return jax.shard_map(
        body, mesh=mesh, in_specs=placed, out_specs=P("front", "panel", None), check_vma=False
    )
```

```python
import functools

import jax
import jax.numpy as jnp
from jax import lax
from jax.experimental import pallas as pl
from jax.experimental.pallas import tpu as pltpu
from jax.sharding import PartitionSpec as P

MAXKIDS = 4
HI = lax.Precision.HIGHEST
MESH = pl.DeviceIdType.MESH


def dot(a, b, dims, precision=None):
    return lax.dot_general(
        a, b, (dims, ((), ())), precision=precision, preferred_element_type=jnp.float32
    )


def level_kernel(steps, picks, counts, coupling_hbm, inverse_hbm, pivots_ref, trailing_hbm, omega_hbm, maps_hbm, tall_hbm, wide_hbm,
                 coupling_ref, inverses, factors, scaled_ref, schur_ref, omega_ref,
                 maps_ref, spots_ref, own_ref, send_sem, recv_sem, local_sem, staged, *rest):
    panel = lax.axis_index("panel")
    chip = panel // 2
    core = panel % 2
    other = 1 - core
    up = (chip + 1) % 4
    down = (chip + 3) % 4
    far = (chip + 2) % 4
    rows, cols = coupling_ref.shape
    half = rows // 2
    chunk = cols // steps
    partner = chip * 2 + other
    above = up * 2 + core
    below = down * 2 + core

    ring, packed, kids, tall, wide = (rest[4 * i:4 * i + 4] for i in range(5))
    fetch_w = pltpu.make_async_copy(inverse_hbm, own_ref, local_sem.at[0])
    fetch_v = pltpu.make_async_copy(inverse_hbm, inverses.at[panel], local_sem.at[13])
    fetch_c = pltpu.make_async_copy(coupling_hbm, coupling_ref, local_sem.at[1])
    fetch_t = pltpu.make_async_copy(trailing_hbm, schur_ref, local_sem.at[2])
    fetch_o = pltpu.make_async_copy(omega_hbm, omega_ref, local_sem.at[3])
    fetch_w.start()
    fetch_v.start()
    fetch_c.start()
    fetch_t.start()
    fetch_m = pltpu.make_async_copy(maps_hbm, maps_ref, local_sem.at[4])
    fetch_o.start()
    fetch_m.start()

    ex = Exchange(picks, packed, ring, staged, kids, rest[20:])
    barrier = pltpu.get_barrier_semaphore()
    for target in (partner, above, below):
        pl.semaphore_signal(barrier, inc=1, device_id={"panel": target}, device_id_type=MESH)
    for target in ex.greeted():
        pl.semaphore_signal(barrier, inc=1, device_id={"front": target}, device_id_type=MESH)
    pl.semaphore_wait(barrier, 8)

    def view(phase, slot, part, c):
        buffer = factors if phase else inverses
        lanes = pl.ds(pl.multiple_of(c * chunk, chunk), chunk)
        if part == 0:
            return buffer.at[slot, :, lanes]
        return buffer.at[slot, pl.ds((part - 1) * half, half), lanes]

    mine = panel
    low = down * 2 + core
    high = up * 2 + core
    table = (
        (mine, 0, partner, partner),
        (mine, 0, above, low),
        (mine, 0, below, high),
        (low, 0, partner, down * 2 + other),
        (high, 0, partner, up * 2 + other),
        (low, 1, above, far * 2 + core),
        (high, 2, below, far * 2 + core),
        (far * 2 + core, 1, partner, far * 2 + other),
        (far * 2 + core, 2, partner, far * 2 + other),
    )

    def copy(phase, kind, c, source=None):
        slot, part, target, _ = table[kind]
        ref = view(phase, slot, part, c)
        return pltpu.make_async_remote_copy(
            src_ref=ref if source is None else source,
            dst_ref=ref,
            send_sem=send_sem.at[phase, c, kind],
            recv_sem=recv_sem.at[phase, c, kind],
            device_id={"panel": target},
            device_id_type=MESH,
        )

    def arrived(phase, kind, c):
        _, part, target, slot = table[kind]
        ref = view(phase, slot, part, c)
        pltpu.make_async_remote_copy(
            src_ref=ref,
            dst_ref=ref,
            send_sem=send_sem.at[phase, c, kind],
            recv_sem=recv_sem.at[phase, c, kind],
            device_id={"panel": target},
            device_id_type=MESH,
        ).wait_recv()

    def lanes_of(c):
        return pl.ds(pl.multiple_of(c * chunk, chunk), chunk)

    def send_inverse(c, carry):
        for kind in (1, 2, 0):
            copy(0, kind, c, own_ref.at[:, lanes_of(c)]).start()
        return carry

    def relay(phase, c):
        arrived(phase, 1, c)
        copy(phase, 5, c).start()
        copy(phase, 3, c).start()
        arrived(phase, 2, c)
        copy(phase, 6, c).start()
        copy(phase, 4, c).start()

    def relay_far(phase, c):
        arrived(phase, 5, c)
        copy(phase, 7, c).start()
        arrived(phase, 6, c)
        copy(phase, 8, c).start()

    def near_inverse(c, carry):
        relay(0, c)
        return carry

    def make_factor(c, carry):
        relay_far(0, c)
        for kind in (0, 3, 4, 7, 8):
            arrived(0, kind, c)
        lanes = lanes_of(c)
        total = dot(coupling_ref[:, :rows], inverses[0, :, lanes], ((1,), (0,)))
        for q in range(1, cols // rows):
            total = total + dot(
                coupling_ref[:, q * rows:(q + 1) * rows], inverses[q, :, lanes], ((1,), (0,))
            )
        factor = total.astype(jnp.bfloat16)
        factors[mine, :, lanes] = factor
        scaled_ref[:, lanes] = (factor.astype(jnp.float32) / pivots_ref[:, lanes]).astype(jnp.bfloat16)
        for kind in (1, 2, 0):
            copy(1, kind, c).start()
        return carry

    def apply(slot, c):
        lanes = lanes_of(c)
        out = pl.ds(pl.multiple_of(slot * rows, rows), rows)
        schur_ref[:, out] -= dot(scaled_ref[:, lanes], factors[slot, :, lanes], ((1,), (1,)))

    def own_tiles(c, carry):
        apply(mine, c)
        arrived(1, 0, c)
        apply(partner, c)
        return carry

    def near_factor(c):
        relay(1, c)
        apply(low, c)
        apply(high, c)
        arrived(1, 3, c)
        apply(down * 2 + other, c)
        arrived(1, 4, c)
        apply(up * 2 + other, c)

    def far_factor(c):
        apply(far * 2 + core, c)
        arrived(1, 7, c)
        arrived(1, 8, c)
        apply(far * 2 + other, c)

    def squeeze(*groups, between=lambda: None):
        tiles = [2 * ((chip + (0, 3, 1, 2)[g]) % 4) + i for g in groups for i in range(2)]
        compress(schur_ref, omega_ref, [packed[g].at[i] for g in groups for i in range(2)], tiles, between)

    def first_hops():
        ex.ring_step(1, 1)
        ex.ring_step(2, 1)

    def spots(s, block, size):
        front = lax.axis_index("front")
        lanes = pl.ds(pl.multiple_of(block * rows, rows), rows)
        where = jnp.where(s < counts[front], maps_ref[pl.ds(picks[front, s], 1), lanes], -1)
        ids = lax.broadcasted_iota(jnp.int32, (size, rows), 0)
        return jnp.where(where == ids, 1.0, 0.0).astype(jnp.bfloat16)

    def row_spots():
        for s in range(MAXKIDS):
            spots_ref[s] = spots(s, panel, spots_ref.shape[1])

    def outward(g, which):
        ref, hbm = ((tall[g], tall_hbm), (wide[g], wide_hbm))[which]
        return pltpu.make_async_copy(ref, hbm.at[ex.tiles[g]], local_sem.at[5 + 2 * g + which])

    def scatter(g):
        ex.pick_wait(g)
        first = 2 * ((chip + (0, 3, 1, 2)[g]) % 4)
        rank = omega_ref.shape[1]
        for s in range(MAXKIDS):
            block = kids[g][s, :, :rank, :].reshape(2 * rank, rows)
            high = dot(block, spots_ref[s], ((1,), (1,))).astype(jnp.bfloat16)
            for i in range(2):
                tall[g][i, s * rank:(s + 1) * rank, :] = high[i * rank:(i + 1) * rank]
                coeff = kids[g][s, i, rank:, :]
                broad = dot(coeff, spots(s, first + i, wide[g].shape[2]), ((1,), (1,)))
                wide[g][i, s * rank:(s + 1) * rank, :] = broad.astype(jnp.bfloat16)
        for which in range(2):
            outward(g, which).start()

    fetch_w.wait()
    lax.fori_loop(0, steps, send_inverse, 0)
    fetch_m.wait()
    row_spots()
    fetch_c.wait()
    fetch_v.wait()
    lax.fori_loop(0, steps, near_inverse, 0)
    lax.fori_loop(0, steps, make_factor, 0)
    fetch_t.wait()
    fetch_o.wait()
    lax.fori_loop(0, steps, own_tiles, 0)
    squeeze(0)
    ex.split_start(0)
    near_factor(0)
    near_factor(1)
    ex.ring_start(0)
    near_factor(2)
    ex.ring_step(0, 1)
    near_factor(3)
    ex.ring_step(0, 2)
    squeeze(1, 2)
    ex.split_start(1)
    ex.split_start(2)
    ex.ring_step(0, 3)
    relay_far(1, 0)
    relay_far(1, 1)
    far_factor(0)
    far_factor(1)
    relay_far(1, 2)
    ex.ring_start(1)
    ex.ring_start(2)
    far_factor(2)
    relay_far(1, 3)
    ex.ring_end(0)
    ex.pick_start(0)
    far_factor(3)
    squeeze(3, between=first_hops)
    ex.split_start(3)
    ex.ring_start(3)
    ex.ring_step(1, 2)
    ex.ring_step(2, 2)
    ex.ring_step(3, 1)
    ex.ring_step(1, 3)
    ex.ring_step(2, 3)
    ex.ring_step(3, 2)
    for g in (1, 2):
        ex.ring_end(g)
        ex.pick_start(g)
    scatter(0)
    ex.ring_step(3, 3)
    scatter(1)
    scatter(2)
    ex.ring_end(3)
    ex.pick_start(3)
    scatter(3)
    for g in range(4):
        ex.drain(g)
        for which in range(2):
            outward(g, which).wait()

    def drain(c, carry):
        for phase in range(2):
            for kind in range(9):
                copy(phase, kind, c).wait_send()
        return carry

    lax.fori_loop(0, steps, drain, 0)


def level(picks, counts, coupling, pivot_inverse, pivots, trailing, omega, maps, height):
    rows, cols = coupling.shape
    tiles, rank, tile = omega.shape
    pieces = cols // rows
    steps = 4
    hbm = pl.BlockSpec(memory_space=pltpu.HBM)
    vmem = pl.BlockSpec(memory_space=pltpu.VMEM)
    spread = (tiles, MAXKIDS * rank, height)
    return pl.pallas_call(
        functools.partial(level_kernel, steps),
        in_specs=[pl.BlockSpec(memory_space=pltpu.SMEM)] * 2 + [hbm, hbm, vmem, hbm, hbm, hbm],
        out_specs=(hbm, hbm),
        out_shape=(jax.ShapeDtypeStruct(spread, jnp.bfloat16),) * 2,
        scratch_shapes=[
            pltpu.VMEM((rows, cols), jnp.bfloat16),
            pltpu.VMEM((pieces, rows, cols), jnp.bfloat16),
            pltpu.VMEM((pieces, rows, cols), jnp.bfloat16),
            pltpu.VMEM((rows, cols), jnp.bfloat16),
            pltpu.VMEM((rows, cols), jnp.float32),
            pltpu.VMEM((tiles, rank, tile), jnp.float32),
            pltpu.VMEM(maps.shape, jnp.int32),
            pltpu.VMEM((MAXKIDS, height, tile), jnp.bfloat16),
            pltpu.VMEM((rows, cols), jnp.bfloat16),
            pltpu.SemaphoreType.DMA((2, steps, 9)),
            pltpu.SemaphoreType.DMA((2, steps, 9)),
            pltpu.SemaphoreType.DMA((14,)),
        ] + exchange_scratch(rank, tile, height),
        name="level",
        compiler_params=pltpu.CompilerParams(
            collective_id=0, has_side_effects=True, vmem_limit_bytes=60 * 1024 * 1024
        ),
    )(picks, counts, coupling, pivot_inverse, pivots, trailing, omega, maps)


def halves(value):
    high = value.astype(jnp.bfloat16)
    return high, (value - high.astype(jnp.float32)).astype(jnp.bfloat16)


def fine(a, b, dims):
    a_high, a_low = halves(a)
    b_high, b_low = halves(b)
    return dot(a_high, b_high, dims) + (dot(a_high, b_low, dims) + dot(a_low, b_high, dims))


def compress(schur_ref, omega_ref, packed, tiles, between):
    _, rank, tile = omega_ref.shape
    ys = []
    state = []
    row_id = lax.broadcasted_iota(jnp.int32, (rank, rank), 0)
    col_id = lax.broadcasted_iota(jnp.int32, (rank, rank), 1)
    eye = jnp.where(row_id == col_id, 1.0, 0.0).astype(jnp.float32)
    spans = [pl.ds(pl.multiple_of(j * tile, tile), tile) for j in tiles]
    for j, span in zip(tiles, spans):
        y = fine(omega_ref[j], schur_ref[:, span], ((1,), (1,)))
        ys.append(y)
        state.append(jnp.concatenate([dot(y, y, ((1,), (1,)), HI), eye], axis=1))
    a = jnp.stack(state)
    rows = lax.broadcasted_iota(jnp.int32, (len(tiles), rank, 1), 1)
    lane = (len(tiles), 1, a.shape[-1])
    first = jnp.broadcast_to(1.0 / a[:, :1, :1], lane)
    for k in range(0, rank, 2):
        col0 = jnp.broadcast_to(jnp.where(rows > k, a[:, :, k:k + 1], 0.0), a.shape)
        col1 = jnp.broadcast_to(jnp.where(rows > k + 1, a[:, :, k + 1:k + 2], 0.0), a.shape)
        cross = col0[:, k + 1:k + 2, :]
        ratio = cross * first
        second = 1.0 / (jnp.broadcast_to(a[:, k + 1:k + 2, k + 1:k + 2], lane) - ratio * cross)
        row0 = a[:, k:k + 1, :]
        row1 = a[:, k + 1:k + 2, :] - ratio * row0
        col1 = jnp.where(rows > k + 1, col1 - col0 * ratio, 0.0)
        scaled0 = row0 * first
        if k + 2 < rank:
            after = jnp.broadcast_to(a[:, k + 2:k + 3, k + 2:k + 3], lane)
            low0 = col0[:, k + 2:k + 3, :]
            low1 = col1[:, k + 2:k + 3, :]
            first = 1.0 / (after - low0 * low0 * first - low1 * low1 * second)
        a = a - col0 * scaled0 - col1 * (row1 * second)
    between()
    for i, (j, span) in enumerate(zip(tiles, spans)):
        diag = jnp.sum(jnp.where(row_id == col_id, a[i, :, :rank], 0.0), axis=1, keepdims=True)
        inverse = a[i, :, rank:] * (1.0 / jnp.sqrt(diag))
        basis = dot(inverse, ys[i], ((1,), (0,)), HI)
        packed[i][:rank, :] = basis.astype(jnp.bfloat16)
        packed[i][rank:, :] = fine(basis, schur_ref[:, span], ((1,), (0,))).astype(jnp.bfloat16)


class Exchange:
    def __init__(self, picks, packed, ring, staged, kids, sems):
        self.picks, self.packed, self.ring, self.staged, self.kids = picks, packed, ring, staged, kids
        self.split_send, self.split_recv, self.ring_send, self.ring_recv, self.pick_send, self.pick_recv, self.own = sems
        front = lax.axis_index("front")
        self.z = front // 4
        self.x = front % 4
        chip = lax.axis_index("panel") // 2
        self.tiles = [pl.ds(pl.multiple_of(2 * ((chip + d) % 4), 2), 2) for d in (0, 3, 1, 2)]

    def across(self, step):
        return self.z * 4 + (self.x + step) % 4

    def greeted(self):
        z = self.z
        return [self.across(s) for s in (1, 2, 3)] + [
            ((z + 1) % 8) * 4 + self.x, ((z + 7) % 8) * 4 + self.x]

    def part(self, x):
        return pl.ds(pl.multiple_of(16 * x, 16), 16)

    def split(self, g, step):
        return pltpu.make_async_remote_copy(
            src_ref=self.packed[g].at[:, self.part((self.x + step) % 4), :],
            dst_ref=self.ring[g].at[self.z, self.x],
            send_sem=self.split_send.at[g, step - 1],
            recv_sem=self.split_recv.at[g, step - 1],
            device_id={"front": self.across(step)},
            device_id_type=MESH,
        )

    def split_own(self, g):
        return pltpu.make_async_copy(
            self.packed[g].at[:, self.part(self.x), :],
            self.ring[g].at[self.z, self.x],
            self.own.at[g],
        )

    def split_start(self, g):
        for step in (2, 1, 3):
            self.split(g, step).start()
        self.split_own(g).start()

    def split_wait(self, g):
        self.split_own(g).wait()
        for step in (1, 3, 2):
            ref = self.ring[g].at[self.z, (self.x + 4 - step) % 4]
            pltpu.make_async_remote_copy(
                src_ref=ref,
                dst_ref=ref,
                send_sem=self.split_send.at[g, step - 1],
                recv_sem=self.split_recv.at[g, step - 1],
                device_id={"front": self.across(step)},
                device_id_type=MESH,
            ).wait_recv()

    def hop(self, g, way, k, incoming):
        sign = -1 if way == 0 else 1
        at = (self.z + 8 + sign * (k + incoming)) % 8
        ref = self.ring[g].at[at]
        if k == 3:
            ref = self.ring[g].at[at, pl.ds(2 * way, 2)]
        target = ((self.z + (1 if way == 0 else 7)) % 8) * 4 + self.x
        return pltpu.make_async_remote_copy(
            src_ref=ref,
            dst_ref=ref,
            send_sem=self.ring_send.at[g, way, k],
            recv_sem=self.ring_recv.at[g, way, k],
            device_id={"front": target},
            device_id_type=MESH,
        )

    def ring_start(self, g):
        self.split_wait(g)
        for way in (0, 1):
            self.hop(g, way, 0, 0).start()

    def ring_step(self, g, k):
        for way in (0, 1):
            self.hop(g, way, k - 1, 1).wait_recv()
            self.hop(g, way, k, 0).start()

    def ring_end(self, g):
        for way in (0, 1):
            self.hop(g, way, 3, 1).wait_recv()

    def pick(self, g, step):
        return pltpu.make_async_remote_copy(
            src_ref=self.staged.at[g, step - 1],
            dst_ref=self.kids[g].at[:, :, self.part(self.x), :],
            send_sem=self.pick_send.at[g, step - 1],
            recv_sem=self.pick_recv.at[g, step - 1],
            device_id={"front": self.across(step)},
            device_id_type=MESH,
        )

    def pick_start(self, g):
        for step in (2, 1, 3, 0):
            for s in range(MAXKIDS):
                child = self.picks[self.across(step), s]
                block = self.ring[g][child // 4, child % 4]
                if step:
                    self.staged[g, step - 1, s] = block
                else:
                    self.kids[g][s, :, self.part(self.x), :] = block
        for step in (2, 1, 3):
            self.pick(g, step).start()

    def pick_wait(self, g):
        for step in (1, 3, 2):
            ref = self.kids[g].at[:, :, self.part((self.x + 4 - step) % 4), :]
            pltpu.make_async_remote_copy(
                src_ref=ref,
                dst_ref=ref,
                send_sem=self.pick_send.at[g, step - 1],
                recv_sem=self.pick_recv.at[g, step - 1],
                device_id={"front": self.across(step)},
                device_id_type=MESH,
            ).wait_recv()

    def drain(self, g):
        for step in (1, 2, 3):
            self.split(g, step).wait_send()
            self.pick(g, step).wait_send()
        for way in (0, 1):
            for k in range(4):
                self.hop(g, way, k, 0).wait_send()


def exchange_scratch(rank, tile, height):
    block = (2, 16, tile)
    shapes = [(8, 4) + block, (2, 2 * rank, tile), (MAXKIDS, 2, 2 * rank, tile)] + [(2, MAXKIDS * rank, height)] * 2
    return [pltpu.VMEM((4, 3, MAXKIDS) + block, jnp.bfloat16)] + [
        pltpu.VMEM(shape, jnp.bfloat16) for shape in shapes for _ in range(4)
    ] + [pltpu.SemaphoreType.DMA(shape) for shape in (
        (4, 3), (4, 3), (4, 2, 4), (4, 2, 4), (4, 3), (4, 3), (4,))]


def place_kernel(parts, tall_hbm, wide_hbm, base_hbm, out_hbm, tall_ref, wide_ref, base_ref, out_ref, sems):
    tiles = tall_ref.shape[0]
    width = wide_ref.shape[2]
    each = tiles // parts
    fetches = []
    for p in range(parts):
        some = pl.ds(p * each, each)
        lanes = pl.ds(p * each * width, each * width)
        fetches.append([
            pltpu.make_async_copy(tall_hbm.at[some], tall_ref.at[some], sems.at[0, p]),
            pltpu.make_async_copy(wide_hbm.at[some], wide_ref.at[some], sems.at[1, p]),
            pltpu.make_async_copy(base_hbm.at[:, lanes], base_ref.at[:, lanes], sems.at[2, p]),
        ])
        for fetch in fetches[p]:
            fetch.start()
    stores = []
    for p in range(parts):
        for fetch in fetches[p]:
            fetch.wait()
        for j in range(p * each, (p + 1) * each):
            lanes = slice(j * width, (j + 1) * width)
            total = dot(tall_ref[j], wide_ref[j], ((0,), (0,)))
            out_ref[:, lanes] = (base_ref[:, lanes].astype(jnp.float32) + total).astype(jnp.bfloat16)
        lanes = pl.ds(p * each * width, each * width)
        store = pltpu.make_async_copy(out_ref.at[:, lanes], out_hbm.at[:, lanes], sems.at[3, p])
        store.start()
        stores.append(store)
    for store in stores:
        store.wait()


def place(tall, wide, base):
    hbm = pl.BlockSpec(memory_space=pltpu.HBM)
    parts = 4
    return pl.pallas_call(
        functools.partial(place_kernel, parts),
        in_specs=[hbm] * 3,
        out_specs=hbm,
        out_shape=jax.ShapeDtypeStruct(base.shape, base.dtype),
        scratch_shapes=[pltpu.VMEM(a.shape, a.dtype) for a in (tall, wide, base, base)]
        + [pltpu.SemaphoreType.DMA((4, parts))],
        name="place",
        compiler_params=pltpu.CompilerParams(vmem_limit_bytes=60 * 1024 * 1024),
    )(tall, wide, base)


def family(parent_of):
    ids = jnp.arange(parent_of.shape[0], dtype=jnp.int32)
    earlier = (parent_of[:, None] == parent_of[None, :]) & (ids[None, :] < ids[:, None])
    position = jnp.sum(earlier.astype(jnp.int32), axis=1)
    takes = parent_of[None, :] == ids[:, None]
    slots = jnp.arange(MAXKIDS, dtype=jnp.int32)
    here = takes[:, None, :] & (position[None, None, :] == slots[None, :, None])
    return jnp.sum(jnp.where(here, ids, 0), axis=2), jnp.sum(takes.astype(jnp.int32), axis=1)


def body(coupling, pivot_inverse, pivots, trailing, sketch, extend_map, parent_of, parent_base):
    picks, counts = family(parent_of)
    tall, wide = level(
        picks, counts, coupling[0], pivot_inverse[0], pivots, trailing[0], sketch[0, 0], extend_map,
        parent_base.shape[1],
    )
    return place(tall, wide, parent_base[0])[None]


def solution(mesh):
    placed = (
        P("front", "panel", None),
        P("front", "panel", None),
        P("front", None),
        P("front", "panel", None),
        P("front", "panel", None, None, None),
        P(),
        P(),
        P("front", "panel", None),
    )
    return jax.shard_map(
        body, mesh=mesh, in_specs=placed, out_specs=P("front", "panel", None), check_vma=False
    )
```

```python
import functools

import jax
import jax.numpy as jnp
from jax import lax
from jax.experimental import pallas as pl
from jax.experimental.pallas import tpu as pltpu
from jax.sharding import PartitionSpec as P

MAXKIDS = 4
HI = lax.Precision.HIGHEST
MESH = pl.DeviceIdType.MESH


def dot(a, b, dims, precision=None):
    return lax.dot_general(
        a, b, (dims, ((), ())), precision=precision, preferred_element_type=jnp.float32
    )


def level_kernel(steps, picks, coupling_hbm, inverse_hbm, pivots_ref, trailing_hbm, omega_hbm, maps_hbm, tall_hbm, wide_hbm,
                 coupling_ref, inverses, factors, scaled_ref, schur_ref, omega_ref,
                 maps_ref, spots_ref, own_ref, send_sem, recv_sem, local_sem, staged, *rest):
    panel = lax.axis_index("panel")
    chip = panel // 2
    core = panel % 2
    other = 1 - core
    up = (chip + 1) % 4
    down = (chip + 3) % 4
    far = (chip + 2) % 4
    rows, cols = coupling_ref.shape
    half = rows // 2
    chunk = cols // steps
    partner = chip * 2 + other
    above = up * 2 + core
    below = down * 2 + core

    ring, packed, kids, tall, wide = (rest[4 * i:4 * i + 4] for i in range(5))
    fetch_w = pltpu.make_async_copy(inverse_hbm, own_ref, local_sem.at[0])
    fetch_v = pltpu.make_async_copy(inverse_hbm, inverses.at[panel], local_sem.at[13])
    fetch_c = pltpu.make_async_copy(coupling_hbm, coupling_ref, local_sem.at[1])
    fetch_t = pltpu.make_async_copy(trailing_hbm, schur_ref, local_sem.at[2])
    fetch_o = pltpu.make_async_copy(omega_hbm, omega_ref, local_sem.at[3])
    fetch_w.start()
    fetch_v.start()
    fetch_c.start()
    fetch_t.start()
    fetch_m = pltpu.make_async_copy(maps_hbm, maps_ref, local_sem.at[4])
    fetch_o.start()
    fetch_m.start()

    ex = Exchange(picks, packed, ring, staged, kids, rest[20:])
    barrier = pltpu.get_barrier_semaphore()
    for target in (partner, above, below):
        pl.semaphore_signal(barrier, inc=1, device_id={"panel": target}, device_id_type=MESH)
    for target in ex.greeted():
        pl.semaphore_signal(barrier, inc=1, device_id={"front": target}, device_id_type=MESH)
    pl.semaphore_wait(barrier, 8)

    def view(phase, slot, part, c):
        buffer = factors if phase else inverses
        lanes = pl.ds(pl.multiple_of(c * chunk, chunk), chunk)
        if part == 0:
            return buffer.at[slot, :, lanes]
        return buffer.at[slot, pl.ds((part - 1) * half, half), lanes]

    mine = panel
    low = down * 2 + core
    high = up * 2 + core
    table = (
        (mine, 0, partner, partner),
        (mine, 0, above, low),
        (mine, 0, below, high),
        (low, 0, partner, down * 2 + other),
        (high, 0, partner, up * 2 + other),
        (low, 1, above, far * 2 + core),
        (high, 2, below, far * 2 + core),
        (far * 2 + core, 1, partner, far * 2 + other),
        (far * 2 + core, 2, partner, far * 2 + other),
    )

    def copy(phase, kind, c, source=None):
        slot, part, target, _ = table[kind]
        ref = view(phase, slot, part, c)
        return pltpu.make_async_remote_copy(
            src_ref=ref if source is None else source,
            dst_ref=ref,
            send_sem=send_sem.at[phase, c, kind],
            recv_sem=recv_sem.at[phase, c, kind],
            device_id={"panel": target},
            device_id_type=MESH,
        )

    def arrived(phase, kind, c):
        _, part, target, slot = table[kind]
        ref = view(phase, slot, part, c)
        pltpu.make_async_remote_copy(
            src_ref=ref,
            dst_ref=ref,
            send_sem=send_sem.at[phase, c, kind],
            recv_sem=recv_sem.at[phase, c, kind],
            device_id={"panel": target},
            device_id_type=MESH,
        ).wait_recv()

    def lanes_of(c):
        return pl.ds(pl.multiple_of(c * chunk, chunk), chunk)

    def send_inverse(c, carry):
        for kind in (1, 2, 0):
            copy(0, kind, c, own_ref.at[:, lanes_of(c)]).start()
        return carry

    def relay(phase, c):
        arrived(phase, 1, c)
        copy(phase, 5, c).start()
        copy(phase, 3, c).start()
        arrived(phase, 2, c)
        copy(phase, 6, c).start()
        copy(phase, 4, c).start()

    def relay_far(phase, c):
        arrived(phase, 5, c)
        copy(phase, 7, c).start()
        arrived(phase, 6, c)
        copy(phase, 8, c).start()

    def near_inverse(c, carry):
        relay(0, c)
        return carry

    def make_factor(c, carry):
        relay_far(0, c)
        for kind in (0, 3, 4, 7, 8):
            arrived(0, kind, c)
        lanes = lanes_of(c)
        total = dot(coupling_ref[:, :rows], inverses[0, :, lanes], ((1,), (0,)))
        for q in range(1, cols // rows):
            total = total + dot(
                coupling_ref[:, q * rows:(q + 1) * rows], inverses[q, :, lanes], ((1,), (0,))
            )
        factor = total.astype(jnp.bfloat16)
        factors[mine, :, lanes] = factor
        scaled_ref[:, lanes] = (factor.astype(jnp.float32) / pivots_ref[:, lanes]).astype(jnp.bfloat16)
        for kind in (1, 2, 0):
            copy(1, kind, c).start()
        return carry

    def apply(slot, c):
        lanes = lanes_of(c)
        out = pl.ds(pl.multiple_of(slot * rows, rows), rows)
        schur_ref[:, out] -= dot(scaled_ref[:, lanes], factors[slot, :, lanes], ((1,), (1,)))

    def own_tiles(c, carry):
        apply(mine, c)
        arrived(1, 0, c)
        apply(partner, c)
        return carry

    def near_factor(c):
        relay(1, c)
        apply(low, c)
        apply(high, c)
        arrived(1, 3, c)
        apply(down * 2 + other, c)
        arrived(1, 4, c)
        apply(up * 2 + other, c)

    def far_factor(c):
        apply(far * 2 + core, c)
        arrived(1, 7, c)
        arrived(1, 8, c)
        apply(far * 2 + other, c)

    def squeeze(*groups, between=lambda: None):
        tiles = [2 * ((chip + (0, 3, 1, 2)[g]) % 4) + i for g in groups for i in range(2)]
        compress(schur_ref, omega_ref, [packed[g].at[i] for g in groups for i in range(2)], tiles, between)

    def first_hops():
        ex.ring_step(1, 1)
        ex.ring_step(2, 1)

    def spots(s, block, size):
        front = lax.axis_index("front")
        lanes = pl.ds(pl.multiple_of(block * rows, rows), rows)
        where = jnp.where(s < picks[front, MAXKIDS], maps_ref[pl.ds(picks[front, s], 1), lanes], -1)
        ids = lax.broadcasted_iota(jnp.int32, (size, rows), 0)
        return jnp.where(where == ids, 1.0, 0.0).astype(jnp.bfloat16)

    def row_spots():
        for s in range(MAXKIDS):
            spots_ref[s] = spots(s, panel, spots_ref.shape[1])

    def outward(g, which):
        ref, hbm = ((tall[g], tall_hbm), (wide[g], wide_hbm))[which]
        return pltpu.make_async_copy(ref, hbm.at[ex.tiles[g]], local_sem.at[5 + 2 * g + which])

    def scatter(g):
        ex.pick_wait(g)
        first = 2 * ((chip + (0, 3, 1, 2)[g]) % 4)
        rank = omega_ref.shape[1]
        for s in range(MAXKIDS):
            block = kids[g][s, :, :rank, :].reshape(2 * rank, rows)
            high = dot(block, spots_ref[s], ((1,), (1,))).astype(jnp.bfloat16)
            for i in range(2):
                tall[g][i, s * rank:(s + 1) * rank, :] = high[i * rank:(i + 1) * rank]
                coeff = kids[g][s, i, rank:, :]
                broad = dot(coeff, spots(s, first + i, wide[g].shape[2]), ((1,), (1,)))
                wide[g][i, s * rank:(s + 1) * rank, :] = broad.astype(jnp.bfloat16)
        for which in range(2):
            outward(g, which).start()

    fetch_w.wait()
    lax.fori_loop(0, steps, send_inverse, 0)
    fetch_m.wait()
    row_spots()
    fetch_c.wait()
    fetch_v.wait()
    lax.fori_loop(0, steps, near_inverse, 0)
    lax.fori_loop(0, steps, make_factor, 0)
    fetch_t.wait()
    fetch_o.wait()
    lax.fori_loop(0, steps, own_tiles, 0)
    squeeze(0)
    ex.split_start(0)
    near_factor(0)
    near_factor(1)
    ex.ring_start(0)
    near_factor(2)
    ex.ring_step(0, 1)
    near_factor(3)
    ex.ring_step(0, 2)
    squeeze(1, 2)
    ex.split_start(1)
    ex.split_start(2)
    ex.ring_step(0, 3)
    relay_far(1, 0)
    relay_far(1, 1)
    far_factor(0)
    far_factor(1)
    relay_far(1, 2)
    ex.ring_start(1)
    ex.ring_start(2)
    far_factor(2)
    relay_far(1, 3)
    ex.ring_end(0)
    ex.pick_start(0)
    far_factor(3)
    squeeze(3, between=first_hops)
    ex.split_start(3)
    scatter(0)
    ex.ring_start(3)
    ex.ring_step(1, 2)
    ex.ring_step(2, 2)
    ex.ring_step(3, 1)
    ex.ring_step(1, 3)
    ex.ring_step(2, 3)
    ex.ring_step(3, 2)
    for g in (1, 2):
        ex.ring_end(g)
        ex.pick_start(g)
    ex.ring_step(3, 3)
    ex.ring_end(3)
    ex.pick_start(3)
    scatter(1)
    scatter(2)
    scatter(3)
    for g in range(4):
        ex.drain(g)
        for which in range(2):
            outward(g, which).wait()

    def drain(c, carry):
        for phase in range(2):
            for kind in range(9):
                copy(phase, kind, c).wait_send()
        return carry

    lax.fori_loop(0, steps, drain, 0)


def level(picks, coupling, pivot_inverse, pivots, trailing, omega, maps, height):
    rows, cols = coupling.shape
    tiles, rank, tile = omega.shape
    pieces = cols // rows
    steps = 4
    hbm = pl.BlockSpec(memory_space=pltpu.HBM)
    vmem = pl.BlockSpec(memory_space=pltpu.VMEM)
    spread = (tiles, MAXKIDS * rank, height)
    return pl.pallas_call(
        functools.partial(level_kernel, steps),
        in_specs=[pl.BlockSpec(memory_space=pltpu.SMEM), hbm, hbm, vmem, hbm, hbm, hbm],
        out_specs=(hbm, hbm),
        out_shape=(jax.ShapeDtypeStruct(spread, jnp.bfloat16),) * 2,
        scratch_shapes=[
            pltpu.VMEM((rows, cols), jnp.bfloat16),
            pltpu.VMEM((pieces, rows, cols), jnp.bfloat16),
            pltpu.VMEM((pieces, rows, cols), jnp.bfloat16),
            pltpu.VMEM((rows, cols), jnp.bfloat16),
            pltpu.VMEM((rows, cols), jnp.float32),
            pltpu.VMEM((tiles, rank, tile), jnp.float32),
            pltpu.VMEM(maps.shape, jnp.int32),
            pltpu.VMEM((MAXKIDS, height, tile), jnp.bfloat16),
            pltpu.VMEM((rows, cols), jnp.bfloat16),
            pltpu.SemaphoreType.DMA((2, steps, 9)),
            pltpu.SemaphoreType.DMA((2, steps, 9)),
            pltpu.SemaphoreType.DMA((14,)),
        ] + exchange_scratch(rank, tile, height),
        name="level",
        compiler_params=pltpu.CompilerParams(
            collective_id=0, has_side_effects=True, vmem_limit_bytes=60 * 1024 * 1024
        ),
    )(picks, coupling, pivot_inverse, pivots, trailing, omega, maps)


def halves(value):
    high = value.astype(jnp.bfloat16)
    return high, (value - high.astype(jnp.float32)).astype(jnp.bfloat16)


def fine(a, b, dims):
    a_high, a_low = halves(a)
    b_high, b_low = halves(b)
    return dot(a_high, b_high, dims) + (dot(a_high, b_low, dims) + dot(a_low, b_high, dims))


def compress(schur_ref, omega_ref, packed, tiles, between):
    _, rank, tile = omega_ref.shape
    ys = []
    state = []
    row_id = lax.broadcasted_iota(jnp.int32, (rank, rank), 0)
    col_id = lax.broadcasted_iota(jnp.int32, (rank, rank), 1)
    eye = jnp.where(row_id == col_id, 1.0, 0.0).astype(jnp.float32)
    spans = [pl.ds(pl.multiple_of(j * tile, tile), tile) for j in tiles]
    for j, span in zip(tiles, spans):
        y = fine(omega_ref[j], schur_ref[:, span], ((1,), (1,)))
        ys.append(y)
        state.append(jnp.concatenate([dot(y, y, ((1,), (1,)), HI), eye], axis=1))
    a = jnp.stack(state)
    rows = lax.broadcasted_iota(jnp.int32, (len(tiles), rank, 1), 1)
    lane = (len(tiles), 1, a.shape[-1])
    first = jnp.broadcast_to(1.0 / a[:, :1, :1], lane)
    for k in range(0, rank, 2):
        col0 = jnp.broadcast_to(jnp.where(rows > k, a[:, :, k:k + 1], 0.0), a.shape)
        col1 = jnp.broadcast_to(jnp.where(rows > k + 1, a[:, :, k + 1:k + 2], 0.0), a.shape)
        cross = col0[:, k + 1:k + 2, :]
        ratio = cross * first
        second = 1.0 / (jnp.broadcast_to(a[:, k + 1:k + 2, k + 1:k + 2], lane) - ratio * cross)
        row0 = a[:, k:k + 1, :]
        row1 = a[:, k + 1:k + 2, :] - ratio * row0
        col1 = jnp.where(rows > k + 1, col1 - col0 * ratio, 0.0)
        scaled0 = row0 * first
        if k + 2 < rank:
            after = jnp.broadcast_to(a[:, k + 2:k + 3, k + 2:k + 3], lane)
            low0 = col0[:, k + 2:k + 3, :]
            low1 = col1[:, k + 2:k + 3, :]
            first = 1.0 / (after - low0 * low0 * first - low1 * low1 * second)
        a = a - col0 * scaled0 - col1 * (row1 * second)
    between()
    for i, (j, span) in enumerate(zip(tiles, spans)):
        diag = jnp.sum(jnp.where(row_id == col_id, a[i, :, :rank], 0.0), axis=1, keepdims=True)
        inverse = a[i, :, rank:] * (1.0 / jnp.sqrt(diag))
        basis = dot(inverse, ys[i], ((1,), (0,)), HI)
        packed[i][:rank, :] = basis.astype(jnp.bfloat16)
        packed[i][rank:, :] = fine(basis, schur_ref[:, span], ((1,), (0,))).astype(jnp.bfloat16)


class Exchange:
    def __init__(self, picks, packed, ring, staged, kids, sems):
        self.picks, self.packed, self.ring, self.staged, self.kids = picks, packed, ring, staged, kids
        self.split_send, self.split_recv, self.ring_send, self.ring_recv, self.pick_send, self.pick_recv, self.own = sems
        front = lax.axis_index("front")
        self.z = front // 4
        self.x = front % 4
        chip = lax.axis_index("panel") // 2
        self.tiles = [pl.ds(pl.multiple_of(2 * ((chip + d) % 4), 2), 2) for d in (0, 3, 1, 2)]

    def across(self, step):
        return self.z * 4 + (self.x + step) % 4

    def greeted(self):
        z = self.z
        return [self.across(s) for s in (1, 2, 3)] + [
            ((z + 1) % 8) * 4 + self.x, ((z + 7) % 8) * 4 + self.x]

    def part(self, x):
        return pl.ds(pl.multiple_of(16 * x, 16), 16)

    def split(self, g, step):
        return pltpu.make_async_remote_copy(
            src_ref=self.packed[g].at[:, self.part((self.x + step) % 4), :],
            dst_ref=self.ring[g].at[self.z, self.x],
            send_sem=self.split_send.at[g, step - 1],
            recv_sem=self.split_recv.at[g, step - 1],
            device_id={"front": self.across(step)},
            device_id_type=MESH,
        )

    def split_own(self, g):
        return pltpu.make_async_copy(
            self.packed[g].at[:, self.part(self.x), :],
            self.ring[g].at[self.z, self.x],
            self.own.at[g],
        )

    def split_start(self, g):
        for step in (2, 1, 3):
            self.split(g, step).start()
        self.split_own(g).start()

    def split_wait(self, g):
        self.split_own(g).wait()
        for step in (1, 3, 2):
            ref = self.ring[g].at[self.z, (self.x + 4 - step) % 4]
            pltpu.make_async_remote_copy(
                src_ref=ref,
                dst_ref=ref,
                send_sem=self.split_send.at[g, step - 1],
                recv_sem=self.split_recv.at[g, step - 1],
                device_id={"front": self.across(step)},
                device_id_type=MESH,
            ).wait_recv()

    def hop(self, g, way, k, incoming):
        sign = -1 if way == 0 else 1
        at = (self.z + 8 + sign * (k + incoming)) % 8
        ref = self.ring[g].at[at]
        if k == 3:
            ref = self.ring[g].at[at, pl.ds(2 * way, 2)]
        target = ((self.z + (1 if way == 0 else 7)) % 8) * 4 + self.x
        return pltpu.make_async_remote_copy(
            src_ref=ref,
            dst_ref=ref,
            send_sem=self.ring_send.at[g, way, k],
            recv_sem=self.ring_recv.at[g, way, k],
            device_id={"front": target},
            device_id_type=MESH,
        )

    def ring_start(self, g):
        self.split_wait(g)
        for way in (0, 1):
            self.hop(g, way, 0, 0).start()

    def ring_step(self, g, k):
        for way in (0, 1):
            self.hop(g, way, k - 1, 1).wait_recv()
            self.hop(g, way, k, 0).start()

    def ring_end(self, g):
        for way in (0, 1):
            self.hop(g, way, 3, 1).wait_recv()

    def pick(self, g, step):
        return pltpu.make_async_remote_copy(
            src_ref=self.staged.at[g, step - 1],
            dst_ref=self.kids[g].at[:, :, self.part(self.x), :],
            send_sem=self.pick_send.at[g, step - 1],
            recv_sem=self.pick_recv.at[g, step - 1],
            device_id={"front": self.across(step)},
            device_id_type=MESH,
        )

    def pick_start(self, g):
        for step in (2, 1, 3, 0):
            for s in range(MAXKIDS):
                child = self.picks[self.across(step), s]
                block = self.ring[g][child // 4, child % 4]
                if step:
                    self.staged[g, step - 1, s] = block
                else:
                    self.kids[g][s, :, self.part(self.x), :] = block
        for step in (2, 1, 3):
            self.pick(g, step).start()

    def pick_wait(self, g):
        for step in (1, 3, 2):
            ref = self.kids[g].at[:, :, self.part((self.x + 4 - step) % 4), :]
            pltpu.make_async_remote_copy(
                src_ref=ref,
                dst_ref=ref,
                send_sem=self.pick_send.at[g, step - 1],
                recv_sem=self.pick_recv.at[g, step - 1],
                device_id={"front": self.across(step)},
                device_id_type=MESH,
            ).wait_recv()

    def drain(self, g):
        for step in (1, 2, 3):
            self.split(g, step).wait_send()
            self.pick(g, step).wait_send()
        for way in (0, 1):
            for k in range(4):
                self.hop(g, way, k, 0).wait_send()


def exchange_scratch(rank, tile, height):
    block = (2, 16, tile)
    shapes = [(8, 4) + block, (2, 2 * rank, tile), (MAXKIDS, 2, 2 * rank, tile)] + [(2, MAXKIDS * rank, height)] * 2
    return [pltpu.VMEM((4, 3, MAXKIDS) + block, jnp.bfloat16)] + [
        pltpu.VMEM(shape, jnp.bfloat16) for shape in shapes for _ in range(4)
    ] + [pltpu.SemaphoreType.DMA(shape) for shape in (
        (4, 3), (4, 3), (4, 2, 4), (4, 2, 4), (4, 3), (4, 3), (4,))]


def place_kernel(parts, tall_hbm, wide_hbm, base_hbm, out_hbm, tall_ref, wide_ref, base_ref, out_ref, sems):
    tiles = tall_ref.shape[0]
    width = wide_ref.shape[2]
    each = tiles // parts
    fetches = []
    for p in range(parts):
        some = pl.ds(p * each, each)
        lanes = pl.ds(p * each * width, each * width)
        fetches.append([
            pltpu.make_async_copy(tall_hbm.at[some], tall_ref.at[some], sems.at[0, p]),
            pltpu.make_async_copy(wide_hbm.at[some], wide_ref.at[some], sems.at[1, p]),
            pltpu.make_async_copy(base_hbm.at[:, lanes], base_ref.at[:, lanes], sems.at[2, p]),
        ])
        for fetch in fetches[p]:
            fetch.start()
    stores = []
    for p in range(parts):
        for fetch in fetches[p]:
            fetch.wait()
        for j in range(p * each, (p + 1) * each):
            lanes = slice(j * width, (j + 1) * width)
            total = dot(tall_ref[j], wide_ref[j], ((0,), (0,)))
            out_ref[:, lanes] = (base_ref[:, lanes].astype(jnp.float32) + total).astype(jnp.bfloat16)
        lanes = pl.ds(p * each * width, each * width)
        store = pltpu.make_async_copy(out_ref.at[:, lanes], out_hbm.at[:, lanes], sems.at[3, p])
        store.start()
        stores.append(store)
    for store in stores:
        store.wait()


def place(tall, wide, base):
    hbm = pl.BlockSpec(memory_space=pltpu.HBM)
    parts = 4
    return pl.pallas_call(
        functools.partial(place_kernel, parts),
        in_specs=[hbm] * 3,
        out_specs=hbm,
        out_shape=jax.ShapeDtypeStruct(base.shape, base.dtype),
        scratch_shapes=[pltpu.VMEM(a.shape, a.dtype) for a in (tall, wide, base, base)]
        + [pltpu.SemaphoreType.DMA((4, parts))],
        name="place",
        compiler_params=pltpu.CompilerParams(vmem_limit_bytes=60 * 1024 * 1024),
    )(tall, wide, base)


def family_kernel(parent_of, picks):
    fronts = parent_of.shape[0]

    def clear(q, carry):
        for s in range(MAXKIDS + 1):
            picks[q, s] = 0
        return carry

    def put(front, carry):
        parent = parent_of[front]
        count = picks[parent, MAXKIDS]
        picks[parent, count] = front
        picks[parent, MAXKIDS] = count + 1
        return carry

    lax.fori_loop(0, fronts, clear, 0, unroll=4)
    lax.fori_loop(0, fronts, put, 0)


def family(parent_of):
    smem = pl.BlockSpec(memory_space=pltpu.SMEM)
    return pl.pallas_call(
        family_kernel,
        in_specs=[smem],
        out_specs=smem,
        out_shape=jax.ShapeDtypeStruct((parent_of.shape[0], MAXKIDS + 1), jnp.int32),
        name="family",
    )(parent_of)


def body(coupling, pivot_inverse, pivots, trailing, sketch, extend_map, parent_of, parent_base):
    picks = family(parent_of)
    tall, wide = level(
        picks, coupling[0], pivot_inverse[0], pivots, trailing[0], sketch[0, 0], extend_map,
        parent_base.shape[1],
    )
    return place(tall, wide, parent_base[0])[None]


def solution(mesh):
    placed = (
        P("front", "panel", None),
        P("front", "panel", None),
        P("front", None),
        P("front", "panel", None),
        P("front", "panel", None, None, None),
        P(),
        P(),
        P("front", "panel", None),
    )
    return jax.shard_map(
        body, mesh=mesh, in_specs=placed, out_specs=P("front", "panel", None), check_vma=False
    )
```
